64 devices in a mesh: dp: 8 (over x, y, core), tp: 8 (over z).
Axes of the slice: x: 2, y: 2, z: 8, core: 2. Of those that a mesh axis runs over, the one named last changes fastest.
The devices are a block of a 4x4x8 slice.
Arguments:
- x: bfloat16 [14336, 5120], P(('dp', 'tp')), parts along dimension 0
- w_gate: bfloat16 [5120, 16384], P(None, 'tp')
- w_up: bfloat16 [5120, 16384], P(None, 'tp')
- w_down: bfloat16 [16384, 5120], P('tp')
Outputs:
- output: bfloat16 [14336, 5120], P(('dp', 'tp')), parts along dimension 0
There are 8 independent parts. The reference program is written for one: setup_inputs(seed, part) draws one part's arguments, and reference() takes and returns one part's arrays. A program takes and returns all parts, laid end to end along the dimension named above; an argument that names none is the same for every part.
All inputs are finite; a program needn't handle non-finite values.
Results may differ from the reference program's by a relative error of at most 0.016.
Values are sent between devices in bfloat16 or wider.
A program may use at most 768 MiB of HBM per device.

```python
import jax
import jax.numpy as jnp

ROWS = 1792
D = 5120
FF = 16384


def setup_inputs(seed: int = 0, part: int = 0) -> dict:
    kx, kg, ku, kd = jax.random.split(jax.random.key(seed), 4)
    drawn = {
        "x": jax.random.normal(jax.random.fold_in(kx, part), (ROWS, D), jnp.float32),
        "w_gate": jax.random.normal(kg, (D, FF), jnp.float32) * D**-0.5,
        "w_up": jax.random.normal(ku, (D, FF), jnp.float32) * D**-0.5,
        "w_down": jax.random.normal(kd, (FF, D), jnp.float32) * FF**-0.5,
    }
    return {k: v.astype(jnp.bfloat16) for k, v in drawn.items()}


def reference(x, w_gate, w_up, w_down):
    gate = jnp.dot(x, w_gate, preferred_element_type=jnp.float32)
    up = jnp.dot(x, w_up, preferred_element_type=jnp.float32)
    hidden = (jax.nn.silu(gate) * up).astype(jnp.bfloat16)
    return jnp.dot(hidden, w_down, preferred_element_type=jnp.float32).astype(jnp.bfloat16)
```

```python
import functools

import jax
import jax.numpy as jnp
from jax import lax
from jax.experimental import pallas as pl
from jax.experimental.pallas import tpu as pltpu
from jax.sharding import PartitionSpec as P

MESH = pl.DeviceIdType.MESH
TILE_UP = 256
TILE_DOWN = 512
PIECE = 1024
DEPTH = 3
ORDER = (5, 7, 3, 6, 1, 4, 2)
AFTER = (None, None, 0, 1, 2, 3, 5)


def mlp_kernel(
    n, x_hbm, wg_hbm, wu_hbm, wd_hbm, y_hbm,
    xbuf, hid, rbuf, wbuf, dbuf,
    x_sem, w_sem, d_sem, y_sem, ag_send, ag_recv, rs_send, rs_recv,
):
    me = lax.axis_index("tp")
    peers = (lax.rem(me + 1, n), lax.rem(me + n - 1, n))
    rows, width = x_hbm.shape
    half = rows // 2
    units = xbuf.shape[0]
    sends = units - 1
    up_tiles = wg_hbm.shape[1] // TILE_UP
    down_tiles = width // TILE_DOWN
    pieces = width // PIECE
    per_piece = PIECE // TILE_DOWN
    top, bottom = pl.ds(0, half), pl.ds(half, half)

    def x_load(h):
        r = pl.ds(h * half, half)
        return pltpu.make_async_copy(x_hbm.at[r], xbuf.at[0, r], x_sem.at[h])

    def w_load(g):
        slot = lax.rem(g, DEPTH)
        cols = pl.ds(pl.multiple_of(lax.rem(g, up_tiles) * TILE_UP, TILE_UP), TILE_UP)
        return (
            pltpu.make_async_copy(wg_hbm.at[:, cols], wbuf.at[slot, :, pl.ds(0, TILE_UP)], w_sem.at[slot, 0]),
            pltpu.make_async_copy(wu_hbm.at[:, cols], wbuf.at[slot, :, pl.ds(TILE_UP, TILE_UP)], w_sem.at[slot, 1]),
        )

    def d_load(q):
        slot = lax.rem(q, DEPTH)
        cols = pl.ds(pl.multiple_of(lax.rem(q, down_tiles) * TILE_DOWN, TILE_DOWN), TILE_DOWN)
        return pltpu.make_async_copy(wd_hbm.at[:, cols], dbuf.at[slot], d_sem.at[slot])

    def gather_copy(k, d, src, dst_unit, dst_rows):
        return pltpu.make_async_remote_copy(
            src_ref=src,
            dst_ref=xbuf.at[dst_unit, dst_rows],
            send_sem=ag_send.at[d, k],
            recv_sem=ag_recv.at[d, k],
            device_id={"tp": peers[d]},
            device_id_type=MESH,
        )

    def sum_copy(r, d, p, src):
        rws = (bottom, top)[d]
        cols = pl.ds(pl.multiple_of(p * PIECE, PIECE), PIECE)
        return pltpu.make_async_remote_copy(
            src_ref=src.at[rws, cols],
            dst_ref=rbuf.at[r, rws, cols],
            send_sem=rs_send.at[d, r, p],
            recv_sem=rs_recv.at[d, r, p],
            device_id={"tp": peers[d]},
            device_id_type=MESH,
        )

    for h in (0, 1):
        x_load(h).start()
    for g in range(DEPTH - 1):
        for c in w_load(g):
            c.start()
    for q in range(DEPTH - 1):
        d_load(q).start()

    barrier = pltpu.get_barrier_semaphore()
    for d in (0, 1):
        pl.semaphore_signal(barrier, inc=1, device_id={"tp": peers[d]}, device_id_type=MESH)
    pl.semaphore_wait(barrier, 2)

    x_load(0).wait()
    gather_copy(0, 0, xbuf.at[0, top], 1, top).start()
    x_load(1).wait()
    gather_copy(0, 1, xbuf.at[0, bottom], 1, bottom).start()
    gather_copy(1, 0, xbuf.at[0, bottom], 2, top).start()
    gather_copy(1, 1, xbuf.at[0, top], 2, bottom).start()

    def hidden(j):
        def tile(t, carry):
            g = j * up_tiles + t
            for c in w_load(g):
                c.wait()

            @pl.when(g + DEPTH - 1 < units * up_tiles)
            def _():
                for c in w_load(g + DEPTH - 1):
                    c.start()

            both = jnp.dot(xbuf[j], wbuf[lax.rem(g, DEPTH)], preferred_element_type=jnp.float32)
            gate, up = both[:, :TILE_UP], both[:, TILE_UP:]
            out = gate * lax.logistic(gate) * up
            hid[j, :, pl.ds(pl.multiple_of(t * TILE_UP, TILE_UP), TILE_UP)] = out.astype(hid.dtype)
            return carry

        lax.fori_loop(0, up_tiles, tile, 0)

    def down(r, u, ready, finish, done):
        def piece(p, carry):
            ready(p)

            def tile(t, c2):
                i = p * per_piece + t
                q = r * down_tiles + i
                d_load(q).wait()

                @pl.when(q + DEPTH - 1 < units * down_tiles)
                def _():
                    d_load(q + DEPTH - 1).start()

                term = jnp.dot(hid[u], dbuf[lax.rem(q, DEPTH)], preferred_element_type=jnp.float32)
                finish(pl.ds(pl.multiple_of(i * TILE_DOWN, TILE_DOWN), TILE_DOWN), term)
                return c2

            lax.fori_loop(0, per_piece, tile, 0)
            done(p)
            return carry

        lax.fori_loop(0, pieces, piece, 0)

    def unit(j, carry):
        @pl.when((j >= 1) & (j < sends))
        def _():
            for d in (0, 1):
                gather_copy(j - 1, d, xbuf.at[0, (top, bottom)[d]], j, (top, bottom)[d]).wait_recv()

        @pl.when(j == sends)
        def _():
            for d in (0, 1):
                gather_copy(j - 1, d, xbuf.at[0, (bottom, top)[d]], j, (bottom, top)[d]).wait_recv()

        @pl.when((j >= 1) & (j < sends - 2))
        def _():
            for d in (0, 1):
                rws = (top, bottom)[d]
                gather_copy(j + 1, d, xbuf.at[j, rws], j + 2, rws).start()

        @pl.when(j == sends - 2)
        def _():
            for d in (0, 1):
                gather_copy(j + 1, d, xbuf.at[j, (top, bottom)[d]], j + 2, (bottom, top)[d]).start()

        hidden(j)

        @pl.when((j == sends - 2) | (j == sends))
        def _():
            r = (j - (sends - 2)) // 2
            for d in (0, 1):
                gather_copy(r + 2, d, xbuf.at[0, (top, bottom)[d]], 1, (top, bottom)[d]).wait_send()

            def finish(cols, term):
                xbuf[r + 1, :, cols] = term.astype(xbuf.dtype)

            def done(p):
                for d in (0, 1):
                    sum_copy(r, d, p, xbuf.at[r + 1]).start()

            down(r, j, lambda p: None, finish, done)

        return carry

    lax.fori_loop(0, units, unit, 0)

    def arrived(slots):
        def wait(p):
            for s in slots:
                for d in (0, 1):
                    sum_copy(s, d, p, rbuf.at[s]).wait_recv()

        return wait

    for r in range(2, sends):
        s = AFTER[r]

        def finish(cols, term, s=s):
            rbuf[s, :, cols] = (rbuf[s, :, cols].astype(jnp.float32) + term).astype(rbuf.dtype)

        def done(p, r=r, s=s):
            for d in (0, 1):
                sum_copy(r, d, p, rbuf.at[s]).start()

        down(r, ORDER[r], arrived((s,)), finish, done)

    for k in (0, 1, 4, 5, 6):
        for d in (0, 1):
            gather_copy(k, d, xbuf.at[0, top], 1, top).wait_send()

    def y_store(p):
        cols = pl.ds(pl.multiple_of(p * PIECE, PIECE), PIECE)
        return pltpu.make_async_copy(xbuf.at[0, :, cols], y_hbm.at[:, cols], y_sem.at[p])

    def finish(cols, term):
        for own, a, b in ((top, bottom, top), (bottom, top, bottom)):
            late = rbuf[6, a, cols].astype(jnp.float32)
            early = rbuf[4, b, cols].astype(jnp.float32)
            lo = 0 if own is top else half
            xbuf[0, own, cols] = (term[lo : lo + half] + early + late).astype(xbuf.dtype)

    down(units - 1, 0, arrived((4, 6)), finish, lambda p: y_store(p).start())

    def drain(p, carry):
        y_store(p).wait()
        for r in range(sends):
            for d in (0, 1):
                sum_copy(r, d, p, rbuf.at[0]).wait_send()
        return carry

    lax.fori_loop(0, pieces, drain, 0)


def solution(mesh):
    n = mesh.shape["tp"]

    def step(x, w_gate, w_up, w_down):
        rows, width = x.shape
        hidden = w_gate.shape[1]
        pieces = width // PIECE
        anywhere = pl.BlockSpec(memory_space=pl.ANY)
        return pl.pallas_call(
            functools.partial(mlp_kernel, n),
            out_shape=jax.ShapeDtypeStruct((rows, width), x.dtype),
            in_specs=[anywhere] * 4,
            out_specs=anywhere,
            scratch_shapes=[
                pltpu.VMEM((n, rows, width), x.dtype),
                pltpu.VMEM((n, rows, hidden), x.dtype),
                pltpu.VMEM((n - 1, rows, width), x.dtype),
                pltpu.VMEM((DEPTH, width, 2 * TILE_UP), x.dtype),
                pltpu.VMEM((DEPTH, hidden, TILE_DOWN), x.dtype),
                pltpu.SemaphoreType.DMA((2,)),
                pltpu.SemaphoreType.DMA((DEPTH, 2)),
                pltpu.SemaphoreType.DMA((DEPTH,)),
                pltpu.SemaphoreType.DMA((pieces,)),
                pltpu.SemaphoreType.DMA((2, n - 1)),
                pltpu.SemaphoreType.DMA((2, n - 1)),
                pltpu.SemaphoreType.DMA((2, n - 1, pieces)),
                pltpu.SemaphoreType.DMA((2, n - 1, pieces)),
            ],
            compiler_params=pltpu.CompilerParams(
                collective_id=0, has_side_effects=True, vmem_limit_bytes=67043328
            ),
            name="mlp_ring",
        )(x, w_gate, w_up, w_down)

    return jax.shard_map(
        step,
        mesh=mesh,
        in_specs=(P(("dp", "tp"), None), P(None, "tp"), P(None, "tp"), P("tp", None)),
        out_specs=P(("dp", "tp"), None),
        check_vma=False,
    )
```

```python
import functools

import jax
import jax.numpy as jnp
from jax import lax
from jax.experimental import pallas as pl
from jax.experimental.pallas import tpu as pltpu
from jax.sharding import PartitionSpec as P

MESH = pl.DeviceIdType.MESH
TILE_UP = 256
TILE_DOWN = 512
PIECE = 1024
DEPTH = 3
KEPT = 4
ORDER = (5, 7, 3, 6, 1, 4, 2)
AFTER = (None, None, 0, 1, 2, 3, 5)


def mlp_kernel(
    n, x_hbm, wg_hbm, wu_hbm, wd_hbm, y_ref,
    xbuf, hid, rbuf, wbuf, dbuf, obuf,
    x_sem, w_sem, d_sem, ag_send, ag_recv, rs_send, rs_recv,
):
    me = lax.axis_index("tp")
    peers = (lax.rem(me + 1, n), lax.rem(me + n - 1, n))
    rows, width = x_hbm.shape
    half = rows // 2
    units = xbuf.shape[0]
    sends = units - 1
    up_tiles = wg_hbm.shape[1] // TILE_UP
    down_tiles = width // TILE_DOWN
    pieces = width // PIECE
    per_piece = PIECE // TILE_DOWN
    top, bottom = pl.ds(0, half), pl.ds(half, half)

    def x_load(h):
        r = pl.ds(h * half, half)
        return pltpu.make_async_copy(x_hbm.at[r], xbuf.at[0, r], x_sem.at[h])

    def w_load(g):
        slot = lax.rem(g, DEPTH)
        cols = pl.ds(pl.multiple_of(lax.rem(g, up_tiles) * TILE_UP, TILE_UP), TILE_UP)
        return (
            pltpu.make_async_copy(wg_hbm.at[:, cols], wbuf.at[slot, :, pl.ds(0, TILE_UP)], w_sem.at[slot, 0]),
            pltpu.make_async_copy(wu_hbm.at[:, cols], wbuf.at[slot, :, pl.ds(TILE_UP, TILE_UP)], w_sem.at[slot, 1]),
        )

    def d_load(q):
        slot = lax.rem(q, DEPTH)
        cols = pl.ds(pl.multiple_of(lax.rem(q, down_tiles) * TILE_DOWN, TILE_DOWN), TILE_DOWN)
        return pltpu.make_async_copy(wd_hbm.at[:, cols], dbuf.at[slot], d_sem.at[slot])

    def gather_copy(k, d, src, dst_unit, dst_rows):
        return pltpu.make_async_remote_copy(
            src_ref=src,
            dst_ref=xbuf.at[dst_unit, dst_rows],
            send_sem=ag_send.at[d, k],
            recv_sem=ag_recv.at[d, k],
            device_id={"tp": peers[d]},
            device_id_type=MESH,
        )

    def landing(r):
        return rbuf.at[r] if r < KEPT else xbuf.at[r - 1]

    def sum_copy(r, d, p, src, dst):
        rws = (bottom, top)[d]
        cols = pl.ds(pl.multiple_of(p * PIECE, PIECE), PIECE)
        return pltpu.make_async_remote_copy(
            src_ref=src.at[rws, cols],
            dst_ref=dst.at[rws, cols],
            send_sem=rs_send.at[d, r, p],
            recv_sem=rs_recv.at[d, r, p],
            device_id={"tp": peers[d]},
            device_id_type=MESH,
        )

    for h in (0, 1):
        x_load(h).start()
    for g in range(DEPTH - 1):
        for c in w_load(g):
            c.start()
    for q in range(DEPTH - 1):
        d_load(q).start()

    barrier = pltpu.get_barrier_semaphore()
    for d in (0, 1):
        pl.semaphore_signal(barrier, inc=1, device_id={"tp": peers[d]}, device_id_type=MESH)
    pl.semaphore_wait(barrier, 2)

    x_load(0).wait()
    gather_copy(0, 0, xbuf.at[0, top], 1, top).start()
    x_load(1).wait()
    gather_copy(0, 1, xbuf.at[0, bottom], 1, bottom).start()
    gather_copy(1, 0, xbuf.at[0, bottom], 2, top).start()
    gather_copy(1, 1, xbuf.at[0, top], 2, bottom).start()

    def hidden(j):
        def tile(t, carry):
            g = j * up_tiles + t
            for c in w_load(g):
                c.wait()

            @pl.when(g + DEPTH - 1 < units * up_tiles)
            def _():
                for c in w_load(g + DEPTH - 1):
                    c.start()

            both = jnp.dot(xbuf[j], wbuf[lax.rem(g, DEPTH)], preferred_element_type=jnp.float32)
            gate, up = both[:, :TILE_UP], both[:, TILE_UP:]
            out = gate * lax.logistic(gate) * up
            hid[j, :, pl.ds(pl.multiple_of(t * TILE_UP, TILE_UP), TILE_UP)] = out.astype(hid.dtype)
            return carry

        lax.fori_loop(0, up_tiles, tile, 0)

    def down(r, u, ready, finish, done):
        def piece(p, carry):
            ready(p)

            def tile(t, c2):
                i = p * per_piece + t
                q = r * down_tiles + i
                d_load(q).wait()

                @pl.when(q + DEPTH - 1 < units * down_tiles)
                def _():
                    d_load(q + DEPTH - 1).start()

                term = jnp.dot(hid[u], dbuf[lax.rem(q, DEPTH)], preferred_element_type=jnp.float32)
                finish(pl.ds(pl.multiple_of(i * TILE_DOWN, TILE_DOWN), TILE_DOWN), term)
                return c2

            lax.fori_loop(0, per_piece, tile, 0)
            done(p)
            return carry

        lax.fori_loop(0, pieces, piece, 0)

    def unit(j, carry):
        @pl.when((j >= 1) & (j < sends))
        def _():
            for d in (0, 1):
                gather_copy(j - 1, d, xbuf.at[0, (top, bottom)[d]], j, (top, bottom)[d]).wait_recv()

        @pl.when(j == sends)
        def _():
            for d in (0, 1):
                gather_copy(j - 1, d, xbuf.at[0, (bottom, top)[d]], j, (bottom, top)[d]).wait_recv()

        @pl.when((j >= 1) & (j < sends - 2))
        def _():
            for d in (0, 1):
                rws = (top, bottom)[d]
                gather_copy(j + 1, d, xbuf.at[j, rws], j + 2, rws).start()

        @pl.when(j == sends - 2)
        def _():
            for d in (0, 1):
                gather_copy(j + 1, d, xbuf.at[j, (top, bottom)[d]], j + 2, (bottom, top)[d]).start()

        hidden(j)

        @pl.when((j == sends - 2) | (j == sends))
        def _():
            r = (j - (sends - 2)) // 2
            for d in (0, 1):
                gather_copy(r + 2, d, xbuf.at[0, (top, bottom)[d]], 1, (top, bottom)[d]).wait_send()

            def finish(cols, term):
                xbuf[r + 1, :, cols] = term.astype(xbuf.dtype)

            def done(p):
                for d in (0, 1):
                    sum_copy(r, d, p, xbuf.at[r + 1], rbuf.at[r]).start()

            down(r, j, lambda p: None, finish, done)

        return carry

    lax.fori_loop(0, units, unit, 0)

    for k in (0, 1, 4, 5, 6):
        for d in (0, 1):
            gather_copy(k, d, xbuf.at[0, top], 1, top).wait_send()

    def arrived(s, p):
        for d in (0, 1):
            sum_copy(s, d, p, landing(s), landing(s)).wait_recv()

    for r in range(2, sends):
        s = AFTER[r]

        def finish(cols, term, s=s):
            total = landing(s)
            total[:, cols] = (total[:, cols].astype(jnp.float32) + term).astype(total.dtype)

        def done(p, r=r, s=s):
            for d in (0, 1):
                sum_copy(r, d, p, landing(s), landing(r)).start()

        down(r, ORDER[r], functools.partial(arrived, s), finish, done)

    def left(lo, hi):
        def drain(p, carry):
            for r in range(lo, hi):
                for d in (0, 1):
                    sum_copy(r, d, p, landing(r), landing(r)).wait_send()
            return carry

        lax.fori_loop(0, pieces, drain, 0)

    left(0, sends - 2)

    early, late = landing(4), landing(6)

    def finish(cols, term):
        obuf[:, pl.ds(pl.multiple_of(lax.rem(cols.start, PIECE), TILE_DOWN), TILE_DOWN)] = term + early[:, cols].astype(jnp.float32)

    def done(p):
        arrived(6, p)
        cols = pl.ds(pl.multiple_of(p * PIECE, PIECE), PIECE)
        for own, other in ((top, bottom), (bottom, top)):
            y_ref[own, cols] = (obuf[own, :] + late[other, cols].astype(jnp.float32)).astype(y_ref.dtype)

    down(units - 1, 0, functools.partial(arrived, 4), finish, done)

    left(sends - 2, sends)


def solution(mesh):
    n = mesh.shape["tp"]

    def step(x, w_gate, w_up, w_down):
        rows, width = x.shape
        hidden = w_gate.shape[1]
        pieces = width // PIECE
        anywhere = pl.BlockSpec(memory_space=pl.ANY)
        return pl.pallas_call(
            functools.partial(mlp_kernel, n),
            out_shape=pltpu.VMEM((rows, width), x.dtype),
            in_specs=[anywhere] * 4,
            out_specs=pl.BlockSpec(memory_space=pltpu.VMEM),
            scratch_shapes=[
                pltpu.VMEM((n, rows, width), x.dtype),
                pltpu.VMEM((n, rows, hidden), x.dtype),
                pltpu.VMEM((KEPT, rows, width), x.dtype),
                pltpu.VMEM((DEPTH, width, 2 * TILE_UP), x.dtype),
                pltpu.VMEM((DEPTH, hidden, TILE_DOWN), x.dtype),
                pltpu.VMEM((rows, PIECE), jnp.float32),
                pltpu.SemaphoreType.DMA((2,)),
                pltpu.SemaphoreType.DMA((DEPTH, 2)),
                pltpu.SemaphoreType.DMA((DEPTH,)),
                pltpu.SemaphoreType.DMA((2, n - 1)),
                pltpu.SemaphoreType.DMA((2, n - 1)),
                pltpu.SemaphoreType.DMA((2, n - 1, pieces)),
                pltpu.SemaphoreType.DMA((2, n - 1, pieces)),
            ],
            compiler_params=pltpu.CompilerParams(
                collective_id=0, has_side_effects=True, vmem_limit_bytes=62000000
            ),
            name="mlp_ring",
        )(x, w_gate, w_up, w_down)

    return jax.shard_map(
        step,
        mesh=mesh,
        in_specs=(P(("dp", "tp"), None), P(None, "tp"), P(None, "tp"), P("tp", None)),
        out_specs=P(("dp", "tp"), None),
        check_vma=False,
    )
```

```python
import functools

import jax
import jax.numpy as jnp
from jax import lax
from jax.experimental import pallas as pl
from jax.experimental.pallas import tpu as pltpu
from jax.sharding import PartitionSpec as P

MESH = pl.DeviceIdType.MESH
TILE_UP = 256
TILE_DOWN = 512
PIECE = 1024
DEPTH = 3
KEPT = 4
ORDER = (5, 7, 3, 6, 1, 4, 2)
AFTER = (None, None, 0, 1, 2, 3, 5)
SPLIT = (0, 1, 5, 6)


def mlp_kernel(
    n, x_hbm, wg_hbm, wu_hbm, wd_hbm, y_ref,
    xbuf, hid, rbuf, wbuf, dbuf, obuf,
    x_sem, w_sem, d_sem, send_sem, ag_recv, rs_recv,
):
    me = lax.axis_index("tp")
    peers = (lax.rem(me + 1, n), lax.rem(me + n - 1, n))
    rows, width = x_hbm.shape
    half = rows // 2
    units = xbuf.shape[0]
    sends = units - 1
    up_tiles = wg_hbm.shape[1] // TILE_UP
    down_tiles = width // TILE_DOWN
    pieces = width // PIECE
    first = (0, pieces, 2 * pieces, 2 * pieces + 1, 2 * pieces + 2, pieces, 0)
    per_piece = PIECE // TILE_DOWN
    top, bottom = pl.ds(0, half), pl.ds(half, half)

    def x_load(h):
        r = pl.ds(h * half, half)
        return pltpu.make_async_copy(x_hbm.at[r], xbuf.at[0, r], x_sem.at[h])

    def w_load(g):
        slot = lax.rem(g, DEPTH)
        cols = pl.ds(pl.multiple_of(lax.rem(g, up_tiles) * TILE_UP, TILE_UP), TILE_UP)
        return (
            pltpu.make_async_copy(wg_hbm.at[:, cols], wbuf.at[slot, :, pl.ds(0, TILE_UP)], w_sem.at[slot]),
            pltpu.make_async_copy(wu_hbm.at[:, cols], wbuf.at[slot, :, pl.ds(TILE_UP, TILE_UP)], w_sem.at[slot]),
        )

    def w_wait(g):
        slot = lax.rem(g, DEPTH)
        pltpu.make_async_copy(wbuf.at[slot], wbuf.at[slot], w_sem.at[slot]).wait()

    def d_load(q):
        slot = lax.rem(q, DEPTH)
        cols = pl.ds(pl.multiple_of(lax.rem(q, down_tiles) * TILE_DOWN, TILE_DOWN), TILE_DOWN)
        return pltpu.make_async_copy(wd_hbm.at[:, cols], dbuf.at[slot], d_sem.at[slot])

    def gather_copy(k, d, src, dst_unit, dst_rows):
        return pltpu.make_async_remote_copy(
            src_ref=src,
            dst_ref=xbuf.at[dst_unit, dst_rows],
            send_sem=send_sem.at[k],
            recv_sem=ag_recv.at[d, lax.rem(k, ag_recv.shape[1])],
            device_id={"tp": peers[d]},
            device_id_type=MESH,
        )

    def sum_copy(r, base, d, p, src, dst):
        rws = (bottom, top)[d]
        cols = pl.ds(0, width) if p is None else pl.ds(pl.multiple_of(p * PIECE, PIECE), PIECE)
        return pltpu.make_async_remote_copy(
            src_ref=src.at[rws, cols],
            dst_ref=dst.at[rws, cols],
            send_sem=send_sem.at[lax.rem(r + 2, sends)],
            recv_sem=rs_recv.at[d, base if p is None else base + p],
            device_id={"tp": peers[d]},
            device_id_type=MESH,
        )

    def landing(r):
        return rbuf.at[r] if r < KEPT else xbuf.at[r - 1]

    def left(k):
        pltpu.make_async_remote_copy(
            src_ref=xbuf.at[0],
            dst_ref=xbuf.at[0],
            send_sem=send_sem.at[k],
            recv_sem=ag_recv.at[0, 0],
            device_id={"tp": peers[0]},
            device_id_type=MESH,
        ).wait_send()

    for h in (0, 1):
        x_load(h).start()
    barrier = pltpu.get_barrier_semaphore()
    for d in (0, 1):
        pl.semaphore_signal(barrier, inc=1, device_id={"tp": peers[d]}, device_id_type=MESH)
    pl.semaphore_wait(barrier, 2)

    x_load(0).wait()
    gather_copy(0, 0, xbuf.at[0, top], 1, top).start()
    x_load(1).wait()
    gather_copy(0, 1, xbuf.at[0, bottom], 1, bottom).start()
    gather_copy(1, 0, xbuf.at[0, bottom], 2, top).start()
    gather_copy(1, 1, xbuf.at[0, top], 2, bottom).start()
    for g in range(DEPTH - 1):
        for c in w_load(g):
            c.start()
    for q in range(DEPTH - 1):
        d_load(q).start()

    def nothing(p):
        return None

    def hidden(j):
        def tile(t, carry):
            g = j * up_tiles + t
            w_wait(g)

            @pl.when(g + DEPTH - 1 < units * up_tiles)
            def _():
                for c in w_load(g + DEPTH - 1):
                    c.start()

            both = jnp.dot(xbuf[j], wbuf[lax.rem(g, DEPTH)], preferred_element_type=jnp.float32)
            gate, up = both[:, :TILE_UP], both[:, TILE_UP:]
            out = gate * lax.logistic(gate) * up
            hid[j, :, pl.ds(pl.multiple_of(t * TILE_UP, TILE_UP), TILE_UP)] = out.astype(hid.dtype)
            return carry

        lax.fori_loop(0, up_tiles, tile, 0)

    def down(r, u, ready, finish, done):
        def piece(p, carry):
            ready(p)

            def tile(t, c2):
                i = p * per_piece + t
                q = r * down_tiles + i
                d_load(q).wait()

                @pl.when(q + DEPTH - 1 < units * down_tiles)
                def _():
                    d_load(q + DEPTH - 1).start()

                term = jnp.dot(hid[u], dbuf[lax.rem(q, DEPTH)], preferred_element_type=jnp.float32)
                finish(pl.ds(pl.multiple_of(i * TILE_DOWN, TILE_DOWN), TILE_DOWN), term)
                return c2

            lax.fori_loop(0, per_piece, tile, 0)
            done(p)
            return carry

        lax.fori_loop(0, pieces, piece, 0)

    def unit(j, carry):
        @pl.when((j >= 1) & (j < sends))
        def _():
            for d in (0, 1):
                gather_copy(j - 1, d, xbuf.at[0, (top, bottom)[d]], j, (top, bottom)[d]).wait_recv()

        @pl.when(j == sends)
        def _():
            for d in (0, 1):
                gather_copy(j - 1, d, xbuf.at[0, (bottom, top)[d]], j, (bottom, top)[d]).wait_recv()

        @pl.when((j >= 1) & (j < sends - 2))
        def _():
            for d in (0, 1):
                rws = (top, bottom)[d]
                gather_copy(j + 1, d, xbuf.at[j, rws], j + 2, rws).start()

        @pl.when(j == sends - 2)
        def _():
            for d in (0, 1):
                gather_copy(j + 1, d, xbuf.at[j, (top, bottom)[d]], j + 2, (bottom, top)[d]).start()

        hidden(j)

        @pl.when((j == sends - 2) | (j == sends))
        def _():
            r = (j - (sends - 2)) // 2
            left(r + 2)

            def finish(cols, term):
                xbuf[r + 1, :, cols] = term.astype(xbuf.dtype)

            def done(p):
                for d in (0, 1):
                    sum_copy(r, r * pieces, d, p, xbuf.at[r + 1], rbuf.at[r]).start()

            down(r, j, nothing, finish, done)

        return carry

    lax.fori_loop(0, units, unit, 0)

    for k in (4, 5, 6, 0, 1):
        left(k)

    def arrived(s, p):
        for d in (0, 1):
            sum_copy(s, first[s], d, p, landing(s), landing(s)).wait_recv()

    def send(r, p):
        for d in (0, 1):
            sum_copy(r, first[r], d, p, landing(AFTER[r]), landing(r)).start()

    for r in range(2, sends):
        s = AFTER[r]

        def finish(cols, term, s=s):
            total = landing(s)
            total[:, cols] = (total[:, cols].astype(jnp.float32) + term).astype(total.dtype)

        if s not in SPLIT:
            arrived(s, None)
        down(
            r,
            ORDER[r],
            functools.partial(arrived, s) if s in SPLIT else nothing,
            finish,
            functools.partial(send, r) if r in SPLIT else nothing,
        )
        if r not in SPLIT:
            send(r, None)

    for r in range(sends - 2):
        left((r + 2) % sends)

    early, late = landing(4), landing(6)

    def finish(cols, term):
        within = pl.ds(pl.multiple_of(lax.rem(cols.start, PIECE), TILE_DOWN), TILE_DOWN)
        obuf[:, within] = term + early[:, cols].astype(jnp.float32)

    def done(p):
        arrived(6, p)
        cols = pl.ds(pl.multiple_of(p * PIECE, PIECE), PIECE)
        for own, other in ((top, bottom), (bottom, top)):
            y_ref[own, cols] = (obuf[own, :] + late[other, cols].astype(jnp.float32)).astype(y_ref.dtype)

    arrived(4, None)
    down(units - 1, 0, nothing, finish, done)
    for r in (sends - 2, sends - 1):
        left((r + 2) % sends)


def solution(mesh):
    n = mesh.shape["tp"]

    def step(x, w_gate, w_up, w_down):
        rows, width = x.shape
        hidden = w_gate.shape[1]
        anywhere = pl.BlockSpec(memory_space=pl.ANY)
        return pl.pallas_call(
            functools.partial(mlp_kernel, n),
            out_shape=pltpu.VMEM((rows, width), x.dtype),
            in_specs=[anywhere] * 4,
            out_specs=pl.BlockSpec(memory_space=pltpu.VMEM),
            scratch_shapes=[
                pltpu.VMEM((n, rows, width), x.dtype),
                pltpu.VMEM((n, rows, hidden), x.dtype),
                pltpu.VMEM((KEPT, rows, width), x.dtype),
                pltpu.VMEM((DEPTH, width, 2 * TILE_UP), x.dtype),
                pltpu.VMEM((DEPTH, hidden, TILE_DOWN), x.dtype),
                pltpu.VMEM((rows, PIECE), jnp.float32),
                pltpu.SemaphoreType.DMA((2,)),
                pltpu.SemaphoreType.DMA((DEPTH,)),
                pltpu.SemaphoreType.DMA((DEPTH,)),
                pltpu.SemaphoreType.DMA((n - 1,)),
                pltpu.SemaphoreType.DMA((2, n // 2)),
                pltpu.SemaphoreType.DMA((2, 2 * (width // PIECE) + 3)),
            ],
            compiler_params=pltpu.CompilerParams(
                collective_id=0, has_side_effects=True, vmem_limit_bytes=62000000
            ),
            name="mlp_ring",
        )(x, w_gate, w_up, w_down)

    return jax.shard_map(
        step,
        mesh=mesh,
        in_specs=(P(("dp", "tp"), None), P(None, "tp"), P(None, "tp"), P("tp", None)),
        out_specs=P(("dp", "tp"), None),
        check_vma=False,
    )
```

```python
import functools

import jax
import jax.numpy as jnp
from jax import lax
from jax.experimental import pallas as pl
from jax.experimental.pallas import tpu as pltpu
from jax.sharding import PartitionSpec as P

MESH = pl.DeviceIdType.MESH
TILE_UP = 256
TILE_DOWN = 512
PIECE = 1024
DEPTH = 3
HEAD = 48
KEPT = 4
ORDER = (5, 7, 3, 6, 1, 4, 2)
AFTER = (None, None, 0, 1, 2, 3, 5)
SPLIT = (0, 1, 5, 6)


def mlp_kernel(
    n, x_hbm, wg_hbm, wu_hbm, wd_hbm, y_ref,
    xbuf, hid, rbuf, wbuf, dbuf, obuf,
    x_sem, w_sem, d_sem, send_sem, ag_recv, rs_recv,
):
    me = lax.axis_index("tp")
    peers = (lax.rem(me + 1, n), lax.rem(me + n - 1, n))
    rows, width = x_hbm.shape
    half = rows // 2
    units = xbuf.shape[0]
    sends = units - 1
    up_tiles = wg_hbm.shape[1] // TILE_UP
    down_tiles = width // TILE_DOWN
    pieces = width // PIECE
    first = (0, pieces, 0, 1, 3, pieces, 0)
    per_piece = PIECE // TILE_DOWN
    top, bottom = pl.ds(0, half), pl.ds(half, half)

    def x_load(h, part):
        rws = pl.ds(h * half + (0, HEAD)[part], (HEAD, half - HEAD)[part])
        return pltpu.make_async_copy(x_hbm.at[rws], xbuf.at[0, rws], x_sem.at[h, part])

    def w_load(g):
        slot = lax.rem(g, DEPTH)
        cols = pl.ds(pl.multiple_of(lax.rem(g, up_tiles) * TILE_UP, TILE_UP), TILE_UP)
        return (
            pltpu.make_async_copy(wg_hbm.at[:, cols], wbuf.at[slot, :, pl.ds(0, TILE_UP)], w_sem.at[slot]),
            pltpu.make_async_copy(wu_hbm.at[:, cols], wbuf.at[slot, :, pl.ds(TILE_UP, TILE_UP)], w_sem.at[slot]),
        )

    def w_wait(g):
        slot = lax.rem(g, DEPTH)
        pltpu.make_async_copy(wbuf.at[slot], wbuf.at[slot], w_sem.at[slot]).wait()

    def d_load(q):
        slot = lax.rem(q, DEPTH)
        cols = pl.ds(pl.multiple_of(lax.rem(q, down_tiles) * TILE_DOWN, TILE_DOWN), TILE_DOWN)
        return pltpu.make_async_copy(wd_hbm.at[:, cols], dbuf.at[slot], d_sem.at[slot])

    def gather_copy(k, d, src, dst_unit, dst_rows):
        return pltpu.make_async_remote_copy(
            src_ref=src,
            dst_ref=xbuf.at[dst_unit, dst_rows],
            send_sem=send_sem.at[k],
            recv_sem=ag_recv.at[d, lax.rem(k, ag_recv.shape[1])],
            device_id={"tp": peers[d]},
            device_id_type=MESH,
        )

    def sum_copy(r, base, d, p, src, dst):
        rws = (bottom, top)[d]
        cols = pl.ds(0, width) if p is None else pl.ds(pl.multiple_of(p * PIECE, PIECE), PIECE)
        return pltpu.make_async_remote_copy(
            src_ref=src.at[rws, cols],
            dst_ref=dst.at[rws, cols],
            send_sem=send_sem.at[lax.rem(r + 2, sends)],
            recv_sem=ag_recv.at[d, base] if p is None else rs_recv.at[d, base + p],
            device_id={"tp": peers[d]},
            device_id_type=MESH,
        )

    def landing(r):
        return rbuf.at[r] if r < KEPT else xbuf.at[r - 1]

    def left(k):
        pltpu.make_async_remote_copy(
            src_ref=xbuf.at[0],
            dst_ref=xbuf.at[0],
            send_sem=send_sem.at[k],
            recv_sem=ag_recv.at[0, 0],
            device_id={"tp": peers[0]},
            device_id_type=MESH,
        ).wait_send()

    barrier = pltpu.get_barrier_semaphore()
    for d in (0, 1):
        pl.semaphore_signal(barrier, inc=1, device_id={"tp": peers[d]}, device_id_type=MESH)
    for part in (0, 1):
        for h in (0, 1):
            x_load(h, part).start()
    pl.semaphore_wait(barrier, 2)

    for part in (0, 1):
        for d in (0, 1):
            x_load(d, part).wait()
            rws = pl.ds(d * half + (0, HEAD)[part], (HEAD, half - HEAD)[part])
            gather_copy(0, d, xbuf.at[0, rws], 1, rws).start()
    gather_copy(1, 0, xbuf.at[0, bottom], 2, top).start()
    gather_copy(1, 1, xbuf.at[0, top], 2, bottom).start()
    for g in range(DEPTH - 1):
        for c in w_load(g):
            c.start()
    for q in range(DEPTH - 1):
        d_load(q).start()

    def nothing(p):
        return None

    def hidden(j):
        def tile(t, carry):
            g = j * up_tiles + t
            w_wait(g)

            @pl.when(g + DEPTH - 1 < units * up_tiles)
            def _():
                for c in w_load(g + DEPTH - 1):
                    c.start()

            both = jnp.dot(xbuf[j], wbuf[lax.rem(g, DEPTH)], preferred_element_type=jnp.float32)
            gate, up = both[:, :TILE_UP], both[:, TILE_UP:]
            out = gate * lax.logistic(gate) * up
            hid[j, :, pl.ds(pl.multiple_of(t * TILE_UP, TILE_UP), TILE_UP)] = out.astype(hid.dtype)
            return carry

        lax.fori_loop(0, up_tiles, tile, 0)

    def down(r, u, ready, finish, done):
        def piece(p, carry):
            ready(p)

            def tile(t, c2):
                i = p * per_piece + t
                q = r * down_tiles + i
                d_load(q).wait()

                @pl.when(q + DEPTH - 1 < units * down_tiles)
                def _():
                    d_load(q + DEPTH - 1).start()

                term = jnp.dot(hid[u], dbuf[lax.rem(q, DEPTH)], preferred_element_type=jnp.float32)
                finish(pl.ds(pl.multiple_of(i * TILE_DOWN, TILE_DOWN), TILE_DOWN), term)
                return c2

            lax.fori_loop(0, per_piece, tile, 0)
            done(p)
            return carry

        lax.fori_loop(0, pieces, piece, 0)

    def unit(j, carry):
        @pl.when((j >= 1) & (j < sends))
        def _():
            for d in (0, 1):
                gather_copy(j - 1, d, xbuf.at[0, (top, bottom)[d]], j, (top, bottom)[d]).wait_recv()

        @pl.when(j == sends)
        def _():
            for d in (0, 1):
                gather_copy(j - 1, d, xbuf.at[0, (bottom, top)[d]], j, (bottom, top)[d]).wait_recv()

        @pl.when((j >= 1) & (j < sends - 2))
        def _():
            for d in (0, 1):
                rws = (top, bottom)[d]
                gather_copy(j + 1, d, xbuf.at[j, rws], j + 2, rws).start()

        @pl.when(j == sends - 2)
        def _():
            for d in (0, 1):
                gather_copy(j + 1, d, xbuf.at[j, (top, bottom)[d]], j + 2, (bottom, top)[d]).start()

        hidden(j)

        @pl.when((j == sends - 2) | (j == sends))
        def _():
            r = (j - (sends - 2)) // 2
            left(r + 2)

            def finish(cols, term):
                xbuf[r + 1, :, cols] = term.astype(xbuf.dtype)

            def done(p):
                for d in (0, 1):
                    sum_copy(r, r * pieces, d, p, xbuf.at[r + 1], rbuf.at[r]).start()

            down(r, j, nothing, finish, done)

        return carry

    lax.fori_loop(0, units, unit, 0)

    for k in (4, 5, 6, 0, 1):
        left(k)

    def arrived(s, p):
        for d in (0, 1):
            sum_copy(s, first[s], d, p, landing(s), landing(s)).wait_recv()

    def send(r, p):
        for d in (0, 1):
            sum_copy(r, first[r], d, p, landing(AFTER[r]), landing(r)).start()

    for r in range(2, sends):
        s = AFTER[r]

        def finish(cols, term, s=s):
            total = landing(s)
            total[:, cols] = (total[:, cols].astype(jnp.float32) + term).astype(total.dtype)

        if s not in SPLIT:
            arrived(s, None)
        down(
            r,
            ORDER[r],
            functools.partial(arrived, s) if s in SPLIT else nothing,
            finish,
            functools.partial(send, r) if r in SPLIT else nothing,
        )
        if r not in SPLIT:
            send(r, None)

    for r in range(sends - 2):
        left((r + 2) % sends)

    early, late = landing(4), landing(6)

    def finish(cols, term):
        within = pl.ds(pl.multiple_of(lax.rem(cols.start, PIECE), TILE_DOWN), TILE_DOWN)
        obuf[:, within] = term + early[:, cols].astype(jnp.float32)

    def done(p):
        arrived(6, p)
        cols = pl.ds(pl.multiple_of(p * PIECE, PIECE), PIECE)
        for own, other in ((top, bottom), (bottom, top)):
            y_ref[own, cols] = (obuf[own, :] + late[other, cols].astype(jnp.float32)).astype(y_ref.dtype)

    arrived(4, None)
    down(units - 1, 0, nothing, finish, done)
    for r in (sends - 2, sends - 1):
        left((r + 2) % sends)


def solution(mesh):
    n = mesh.shape["tp"]

    def step(x, w_gate, w_up, w_down):
        rows, width = x.shape
        hidden = w_gate.shape[1]
        anywhere = pl.BlockSpec(memory_space=pl.ANY)
        return pl.pallas_call(
            functools.partial(mlp_kernel, n),
            out_shape=pltpu.VMEM((rows, width), x.dtype),
            in_specs=[anywhere] * 4,
            out_specs=pl.BlockSpec(memory_space=pltpu.VMEM),
            scratch_shapes=[
                pltpu.VMEM((n, rows, width), x.dtype),
                pltpu.VMEM((n, rows, hidden), x.dtype),
                pltpu.VMEM((KEPT, rows, width), x.dtype),
                pltpu.VMEM((DEPTH, width, 2 * TILE_UP), x.dtype),
                pltpu.VMEM((DEPTH, hidden, TILE_DOWN), x.dtype),
                pltpu.VMEM((rows, PIECE), jnp.float32),
                pltpu.SemaphoreType.DMA((2, 2)),
                pltpu.SemaphoreType.DMA((DEPTH,)),
                pltpu.SemaphoreType.DMA((DEPTH,)),
                pltpu.SemaphoreType.DMA((n - 1,)),
                pltpu.SemaphoreType.DMA((2, n // 2)),
                pltpu.SemaphoreType.DMA((2, 2 * (width // PIECE))),
            ],
            compiler_params=pltpu.CompilerParams(
                collective_id=0, has_side_effects=True, vmem_limit_bytes=62000000
            ),
            name="mlp_ring",
        )(x, w_gate, w_up, w_down)

    return jax.shard_map(
        step,
        mesh=mesh,
        in_specs=(P(("dp", "tp"), None), P(None, "tp"), P(None, "tp"), P("tp", None)),
        out_specs=P(("dp", "tp"), None),
        check_vma=False,
    )
```

```python
import functools

import jax
import jax.numpy as jnp
from jax import lax
from jax.experimental import pallas as pl
from jax.experimental.pallas import tpu as pltpu
from jax.sharding import PartitionSpec as P

MESH = pl.DeviceIdType.MESH
TILE_UP = 256
TILE_DOWN = 512
PIECES = (5, 4, 1)
DEPTH = 3
HEAD = 48
KEPT = 4
ORDER = (5, 7, 3, 6, 1, 4, 2)
AFTER = (None, None, 0, 1, 2, 3, 5)
SPLIT = (0, 1, 5, 6)


def mlp_kernel(
    n, x_hbm, wg_hbm, wu_hbm, wd_hbm, y_ref,
    xbuf, hid, rbuf, wbuf, dbuf, obuf,
    w_sem, d_sem, send_sem, ag_recv, rs_recv,
):
    me = lax.axis_index("tp")
    peers = (lax.rem(me + 1, n), lax.rem(me + n - 1, n))
    rows, width = x_hbm.shape
    half = rows // 2
    units = xbuf.shape[0]
    sends = units - 1
    up_tiles = wg_hbm.shape[1] // TILE_UP
    down_tiles = width // TILE_DOWN
    pieces = len(PIECES)
    starts = tuple(sum(PIECES[:p]) for p in range(pieces))
    first = (0, pieces, 0, 1, 3, pieces, 0)
    gather_left, sum_left = (0, 0, 1, 2, 3, 3, 3), (1, 2, 3, 3, 3, 0, 0)
    top, bottom = pl.ds(0, half), pl.ds(half, half)

    def x_load(h, part):
        rws = pl.ds(h * half + (0, HEAD)[part], (HEAD, half - HEAD)[part])
        return pltpu.make_async_copy(x_hbm.at[rws], xbuf.at[0, rws], (w_sem, d_sem)[h].at[part])

    def w_load(g):
        slot = lax.rem(g, DEPTH)
        cols = pl.ds(pl.multiple_of(lax.rem(g, up_tiles) * TILE_UP, TILE_UP), TILE_UP)
        return (
            pltpu.make_async_copy(wg_hbm.at[:, cols], wbuf.at[slot, :, pl.ds(0, TILE_UP)], w_sem.at[slot]),
            pltpu.make_async_copy(wu_hbm.at[:, cols], wbuf.at[slot, :, pl.ds(TILE_UP, TILE_UP)], w_sem.at[slot]),
        )

    def w_wait(g):
        slot = lax.rem(g, DEPTH)
        pltpu.make_async_copy(wbuf.at[slot], wbuf.at[slot], w_sem.at[slot]).wait()

    def d_load(q):
        slot = lax.rem(q, DEPTH)
        cols = pl.ds(pl.multiple_of(lax.rem(q, down_tiles) * TILE_DOWN, TILE_DOWN), TILE_DOWN)
        return pltpu.make_async_copy(wd_hbm.at[:, cols], dbuf.at[slot], d_sem.at[slot])

    def gather_copy(k, d, src, dst_unit, dst_rows, sem=None):
        return pltpu.make_async_remote_copy(
            src_ref=src,
            dst_ref=xbuf.at[dst_unit, dst_rows],
            send_sem=send_sem.at[gather_left[k] if sem is None else sem],
            recv_sem=ag_recv.at[d, lax.rem(k, ag_recv.shape[1])],
            device_id={"tp": peers[d]},
            device_id_type=MESH,
        )

    def sum_copy(base, sem, d, p, src, dst):
        rws = (bottom, top)[d]
        cols = pl.ds(0, width) if p is None else pl.ds(starts[p] * TILE_DOWN, PIECES[p] * TILE_DOWN)
        return pltpu.make_async_remote_copy(
            src_ref=src.at[rws, cols],
            dst_ref=dst.at[rws, cols],
            send_sem=send_sem.at[sem],
            recv_sem=ag_recv.at[d, base] if p is None else rs_recv.at[d, base + p],
            device_id={"tp": peers[d]},
            device_id_type=MESH,
        )

    def landing(r):
        return rbuf.at[r] if r < KEPT else xbuf.at[r - 1]

    def left(sem, blocks):
        pltpu.make_async_remote_copy(
            src_ref=xbuf.at[pl.ds(0, blocks)],
            dst_ref=xbuf.at[pl.ds(0, blocks)],
            send_sem=send_sem.at[sem],
            recv_sem=ag_recv.at[0, 0],
            device_id={"tp": peers[0]},
            device_id_type=MESH,
        ).wait_send()

    barrier = pltpu.get_barrier_semaphore()
    for d in (0, 1):
        pl.semaphore_signal(barrier, inc=1, device_id={"tp": peers[d]}, device_id_type=MESH)
    for part in (0, 1):
        for h in (0, 1):
            x_load(h, part).start()
    pl.semaphore_wait(barrier, 2)

    for part in (0, 1):
        for d in (0, 1):
            x_load(d, part).wait()
            rws = pl.ds(d * half + (0, HEAD)[part], (HEAD, half - HEAD)[part])
            gather_copy(0, d, xbuf.at[0, rws], 1, rws).start()
    gather_copy(1, 0, xbuf.at[0, bottom], 2, top).start()
    gather_copy(1, 1, xbuf.at[0, top], 2, bottom).start()
    for g in range(DEPTH - 1):
        for c in w_load(g):
            c.start()
    for q in range(DEPTH - 1):
        d_load(q).start()

    def nothing(p):
        return None

    def hidden(j):
        def tile(t, carry):
            g = j * up_tiles + t
            w_wait(g)

            @pl.when(g + DEPTH - 1 < units * up_tiles)
            def _():
                for c in w_load(g + DEPTH - 1):
                    c.start()

            both = jnp.dot(xbuf[j], wbuf[lax.rem(g, DEPTH)], preferred_element_type=jnp.float32)
            gate, up = both[:, :TILE_UP], both[:, TILE_UP:]
            out = gate * lax.logistic(gate) * up
            hid[j, :, pl.ds(pl.multiple_of(t * TILE_UP, TILE_UP), TILE_UP)] = out.astype(hid.dtype)
            return carry

        lax.fori_loop(0, up_tiles, tile, 0)

    def down(r, u, ready, finish, done):
        for p in range(pieces):
            ready(p)

            def tile(t, carry, p=p):
                i = starts[p] + t
                q = r * down_tiles + i
                d_load(q).wait()

                @pl.when(q + DEPTH - 1 < units * down_tiles)
                def _():
                    d_load(q + DEPTH - 1).start()

                term = jnp.dot(hid[u], dbuf[lax.rem(q, DEPTH)], preferred_element_type=jnp.float32)
                finish(pl.ds(pl.multiple_of(i * TILE_DOWN, TILE_DOWN), TILE_DOWN), term, t)
                return carry

            lax.fori_loop(0, PIECES[p], tile, 0)
            done(p)

    def unit(j, carry):
        @pl.when((j >= 1) & (j < sends))
        def _():
            for d in (0, 1):
                gather_copy(j - 1, d, xbuf.at[0, (top, bottom)[d]], j, (top, bottom)[d], 0).wait_recv()

        @pl.when(j == sends)
        def _():
            for d in (0, 1):
                gather_copy(j - 1, d, xbuf.at[0, (bottom, top)[d]], j, (bottom, top)[d], 0).wait_recv()

        for lo, hi in ((1, 3), (3, sends - 2)):

            @pl.when((j >= lo) & (j < hi))
            def _(lo=lo):
                sem = j if lo == 1 else 3
                for d in (0, 1):
                    rws = (top, bottom)[d]
                    gather_copy(j + 1, d, xbuf.at[j, rws], j + 2, rws, sem).start()

        @pl.when(j == sends - 2)
        def _():
            for d in (0, 1):
                gather_copy(j + 1, d, xbuf.at[j, (top, bottom)[d]], j + 2, (bottom, top)[d], 3).start()

        hidden(j)

        @pl.when((j == sends - 2) | (j == sends))
        def _():
            r = (j - (sends - 2)) // 2
            left(r + 1, 1)

            def finish(cols, term, t):
                xbuf[r + 1, :, cols] = term.astype(xbuf.dtype)

            def done(p):
                for d in (0, 1):
                    sum_copy(r * pieces, r + 1, d, p, xbuf.at[r + 1], rbuf.at[r]).start()

            down(r, j, nothing, finish, done)

        return carry

    lax.fori_loop(0, units, unit, 0)

    left(0, 2)
    left(3, 3)

    def arrived(s, p):
        for d in (0, 1):
            sum_copy(first[s], sum_left[s], d, p, landing(s), landing(s)).wait_recv()

    def send(r, p):
        for d in (0, 1):
            sum_copy(first[r], sum_left[r], d, p, landing(AFTER[r]), landing(r)).start()

    for r in range(2, sends):
        s = AFTER[r]

        def finish(cols, term, t, s=s):
            total = landing(s)
            total[:, cols] = (total[:, cols].astype(jnp.float32) + term).astype(total.dtype)

        if s not in SPLIT:
            arrived(s, None)
        down(
            r,
            ORDER[r],
            functools.partial(arrived, s) if s in SPLIT else nothing,
            finish,
            functools.partial(send, r) if r in SPLIT else nothing,
        )
        if r not in SPLIT:
            send(r, None)

    left(1, 1)
    left(2, 1)
    left(3, 3)

    early, late = landing(4), landing(6)

    def finish(cols, term, t):
        within = pl.ds(pl.multiple_of(t * TILE_DOWN, TILE_DOWN), TILE_DOWN)
        obuf[:, within] = term + early[:, cols].astype(jnp.float32)

    def done(p):
        arrived(6, p)
        size = PIECES[p] * TILE_DOWN
        cols = pl.ds(starts[p] * TILE_DOWN, size)
        for own, other in ((top, bottom), (bottom, top)):
            y_ref[own, cols] = (obuf[own, pl.ds(0, size)] + late[other, cols].astype(jnp.float32)).astype(y_ref.dtype)

    arrived(4, None)
    down(units - 1, 0, nothing, finish, done)
    left(0, 2)


def solution(mesh):
    n = mesh.shape["tp"]

    def step(x, w_gate, w_up, w_down):
        rows, width = x.shape
        hidden = w_gate.shape[1]
        anywhere = pl.BlockSpec(memory_space=pl.ANY)
        return pl.pallas_call(
            functools.partial(mlp_kernel, n),
            out_shape=pltpu.VMEM((rows, width), x.dtype),
            in_specs=[anywhere] * 4,
            out_specs=pl.BlockSpec(memory_space=pltpu.VMEM),
            scratch_shapes=[
                pltpu.VMEM((n, rows, width), x.dtype),
                pltpu.VMEM((n, rows, hidden), x.dtype),
                pltpu.VMEM((KEPT, rows, width), x.dtype),
                pltpu.VMEM((DEPTH, width, 2 * TILE_UP), x.dtype),
                pltpu.VMEM((DEPTH, hidden, TILE_DOWN), x.dtype),
                pltpu.VMEM((rows, max(PIECES) * TILE_DOWN), jnp.float32),
                pltpu.SemaphoreType.DMA((DEPTH,)),
                pltpu.SemaphoreType.DMA((DEPTH,)),
                pltpu.SemaphoreType.DMA((4,)),
                pltpu.SemaphoreType.DMA((2, n // 2)),
                pltpu.SemaphoreType.DMA((2, 2 * len(PIECES))),
            ],
            compiler_params=pltpu.CompilerParams(
                collective_id=0, has_side_effects=True, vmem_limit_bytes=62000000
            ),
            name="mlp_ring",
        )(x, w_gate, w_up, w_down)

    return jax.shard_map(
        step,
        mesh=mesh,
        in_specs=(P(("dp", "tp"), None), P(None, "tp"), P(None, "tp"), P("tp", None)),
        out_specs=P(("dp", "tp"), None),
        check_vma=False,
    )
```

```python
import functools

import jax
import jax.numpy as jnp
from jax import lax
from jax.experimental import pallas as pl
from jax.experimental.pallas import tpu as pltpu
from jax.sharding import PartitionSpec as P

MESH = pl.DeviceIdType.MESH
TILE_UP = 256
TILE_DOWN = 512
PIECES = (5, 4, 1)
DEPTH = 3
HEAD = 48
KEPT = 4
ORDER = (5, 7, 3, 6, 1, 4, 2)
AFTER = (None, None, 0, 1, 2, 3, 5)
SPLIT = (0, 1, 5, 6)


def mlp_kernel(
    n, x_hbm, wg_hbm, wu_hbm, wd_hbm, y_ref,
    xbuf, hid, rbuf, wbuf, dbuf, obuf,
    w_sem, d_sem, send_sem, ag_recv, rs_recv,
):
    me = lax.axis_index("tp")
    peers = (lax.rem(me + 1, n), lax.rem(me + n - 1, n))
    rows, width = x_hbm.shape
    half = rows // 2
    units = xbuf.shape[0]
    sends = units - 1
    up_tiles = wg_hbm.shape[1] // TILE_UP
    down_tiles = width // TILE_DOWN
    pieces = len(PIECES)
    starts = tuple(sum(PIECES[:p]) for p in range(pieces))
    first = (0, pieces, 0, 1, 3, pieces, 0)
    gather_left, sum_left = (0, 0, 1, 2, 3, 3, 3), (1, 2, 3, 3, 3, 0, 0)
    top, bottom = pl.ds(0, half), pl.ds(half, half)

    def x_load(h, part):
        rws = pl.ds(h * half + (0, HEAD)[part], (HEAD, half - HEAD)[part])
        return pltpu.make_async_copy(x_hbm.at[rws], xbuf.at[0, rws], (w_sem, d_sem)[h].at[part])

    def w_load(g):
        slot = lax.rem(g, DEPTH)
        cols = pl.ds(pl.multiple_of(lax.rem(g, up_tiles) * TILE_UP, TILE_UP), TILE_UP)
        return (
            pltpu.make_async_copy(wg_hbm.at[:, cols], wbuf.at[slot, :, pl.ds(0, TILE_UP)], w_sem.at[slot]),
            pltpu.make_async_copy(wu_hbm.at[:, cols], wbuf.at[slot, :, pl.ds(TILE_UP, TILE_UP)], w_sem.at[slot]),
        )

    def w_wait(g):
        slot = lax.rem(g, DEPTH)
        pltpu.make_async_copy(wbuf.at[slot], wbuf.at[slot], w_sem.at[slot]).wait()

    def d_load(q):
        slot = lax.rem(q, DEPTH)
        cols = pl.ds(pl.multiple_of(lax.rem(q, down_tiles) * TILE_DOWN, TILE_DOWN), TILE_DOWN)
        return pltpu.make_async_copy(wd_hbm.at[:, cols], dbuf.at[slot], d_sem.at[slot])

    def gather_copy(k, d, src, dst_unit, dst_rows, sem=None):
        return pltpu.make_async_remote_copy(
            src_ref=src,
            dst_ref=xbuf.at[dst_unit, dst_rows],
            send_sem=send_sem.at[gather_left[k] if sem is None else sem],
            recv_sem=ag_recv.at[lax.rem(k, ag_recv.shape[0])],
            device_id={"tp": peers[d]},
            device_id_type=MESH,
        )

    def sum_copy(base, sem, d, p, src, dst):
        rws = (bottom, top, pl.ds(0, rows))[d]
        cols = pl.ds(0, width) if p is None else pl.ds(starts[p] * TILE_DOWN, PIECES[p] * TILE_DOWN)
        return pltpu.make_async_remote_copy(
            src_ref=src.at[rws, cols],
            dst_ref=dst.at[rws, cols],
            send_sem=send_sem.at[sem],
            recv_sem=ag_recv.at[base] if p is None else rs_recv.at[base + p],
            device_id={"tp": peers[d % 2]},
            device_id_type=MESH,
        )

    def landing(r):
        return rbuf.at[r] if r < KEPT else xbuf.at[r - 1]

    def left(sem, blocks):
        pltpu.make_async_remote_copy(
            src_ref=xbuf.at[pl.ds(0, blocks)],
            dst_ref=xbuf.at[pl.ds(0, blocks)],
            send_sem=send_sem.at[sem],
            recv_sem=ag_recv.at[0],
            device_id={"tp": peers[0]},
            device_id_type=MESH,
        ).wait_send()

    barrier = pltpu.get_barrier_semaphore()
    for d in (0, 1):
        pl.semaphore_signal(barrier, inc=1, device_id={"tp": peers[d]}, device_id_type=MESH)
    for part in (0, 1):
        for h in (0, 1):
            x_load(h, part).start()
    pl.semaphore_wait(barrier, 2)

    for part in (0, 1):
        for d in (0, 1):
            x_load(d, part).wait()
            rws = pl.ds(d * half + (0, HEAD)[part], (HEAD, half - HEAD)[part])
            gather_copy(0, d, xbuf.at[0, rws], 1, rws).start()
    gather_copy(1, 0, xbuf.at[0, bottom], 2, top).start()
    gather_copy(1, 1, xbuf.at[0, top], 2, bottom).start()
    for g in range(DEPTH - 1):
        for c in w_load(g):
            c.start()
    for q in range(DEPTH - 1):
        d_load(q).start()

    def nothing(p):
        return None

    def hidden(j):
        def tile(t, carry):
            g = j * up_tiles + t
            w_wait(g)

            @pl.when(g + DEPTH - 1 < units * up_tiles)
            def _():
                for c in w_load(g + DEPTH - 1):
                    c.start()

            both = jnp.dot(xbuf[j], wbuf[lax.rem(g, DEPTH)], preferred_element_type=jnp.float32)
            gate, up = both[:, :TILE_UP], both[:, TILE_UP:]
            out = gate * lax.logistic(gate) * up
            hid[j, :, pl.ds(pl.multiple_of(t * TILE_UP, TILE_UP), TILE_UP)] = out.astype(hid.dtype)
            return carry

        lax.fori_loop(0, up_tiles, tile, 0)

    def down(r, u, ready, finish, done):
        for p in range(pieces):
            ready(p)

            def tile(t, carry, p=p):
                i = starts[p] + t
                q = r * down_tiles + i
                d_load(q).wait()

                @pl.when(q + DEPTH - 1 < units * down_tiles)
                def _():
                    d_load(q + DEPTH - 1).start()

                term = jnp.dot(hid[u], dbuf[lax.rem(q, DEPTH)], preferred_element_type=jnp.float32)
                finish(pl.ds(pl.multiple_of(i * TILE_DOWN, TILE_DOWN), TILE_DOWN), term, t)
                return carry

            lax.fori_loop(0, PIECES[p], tile, 0)
            done(p)

    def unit(j, carry):
        @pl.when(j >= 1)
        def _():
            gather_copy(j - 1, 0, xbuf.at[0], j, pl.ds(0, rows), 0).wait_recv()

        for lo, hi in ((1, 3), (3, sends - 2)):

            @pl.when((j >= lo) & (j < hi))
            def _(lo=lo):
                sem = j if lo == 1 else 3
                for d in (0, 1):
                    rws = (top, bottom)[d]
                    gather_copy(j + 1, d, xbuf.at[j, rws], j + 2, rws, sem).start()

        @pl.when(j == sends - 2)
        def _():
            for d in (0, 1):
                gather_copy(j + 1, d, xbuf.at[j, (top, bottom)[d]], j + 2, (bottom, top)[d], 3).start()

        hidden(j)

        @pl.when((j == sends - 2) | (j == sends))
        def _():
            r = (j - (sends - 2)) // 2
            left(r + 1, 1)

            def finish(cols, term, t):
                xbuf[r + 1, :, cols] = term.astype(xbuf.dtype)

            def done(p):
                for d in (0, 1):
                    sum_copy(r * pieces, r + 1, d, p, xbuf.at[r + 1], rbuf.at[r]).start()

            down(r, j, nothing, finish, done)

        return carry

    lax.fori_loop(0, units, unit, 0)

    left(0, 2)
    left(3, 3)

    def arrived(s, p):
        sum_copy(first[s], sum_left[s], 2, p, landing(s), landing(s)).wait_recv()

    def send(r, p):
        for d in (0, 1):
            sum_copy(first[r], sum_left[r], d, p, landing(AFTER[r]), landing(r)).start()

    for r in range(2, sends):
        s = AFTER[r]

        def finish(cols, term, t, s=s):
            total = landing(s)
            total[:, cols] = (total[:, cols].astype(jnp.float32) + term).astype(total.dtype)

        if s not in SPLIT:
            arrived(s, None)
        down(
            r,
            ORDER[r],
            functools.partial(arrived, s) if s in SPLIT else nothing,
            finish,
            functools.partial(send, r) if r in SPLIT else nothing,
        )
        if r not in SPLIT:
            send(r, None)

    left(1, 1)
    left(2, 1)
    left(3, 3)

    early, late = landing(4), landing(6)

    def finish(cols, term, t):
        within = pl.ds(pl.multiple_of(t * TILE_DOWN, TILE_DOWN), TILE_DOWN)
        obuf[:, within] = term + early[:, cols].astype(jnp.float32)

    def done(p):
        arrived(6, p)
        size = PIECES[p] * TILE_DOWN
        cols = pl.ds(starts[p] * TILE_DOWN, size)
        for own, other in ((top, bottom), (bottom, top)):
            y_ref[own, cols] = (obuf[own, pl.ds(0, size)] + late[other, cols].astype(jnp.float32)).astype(y_ref.dtype)

    arrived(4, None)
    down(units - 1, 0, nothing, finish, done)
    left(0, 2)


def solution(mesh):
    n = mesh.shape["tp"]

    def step(x, w_gate, w_up, w_down):
        rows, width = x.shape
        hidden = w_gate.shape[1]
        anywhere = pl.BlockSpec(memory_space=pl.ANY)
        return pl.pallas_call(
            functools.partial(mlp_kernel, n),
            out_shape=pltpu.VMEM((rows, width), x.dtype),
            in_specs=[anywhere] * 4,
            out_specs=pl.BlockSpec(memory_space=pltpu.VMEM),
            scratch_shapes=[
                pltpu.VMEM((n, rows, width), x.dtype),
                pltpu.VMEM((n, rows, hidden), x.dtype),
                pltpu.VMEM((KEPT, rows, width), x.dtype),
                pltpu.VMEM((DEPTH, width, 2 * TILE_UP), x.dtype),
                pltpu.VMEM((DEPTH, hidden, TILE_DOWN), x.dtype),
                pltpu.VMEM((rows, max(PIECES) * TILE_DOWN), jnp.float32),
                pltpu.SemaphoreType.DMA((DEPTH,)),
                pltpu.SemaphoreType.DMA((DEPTH,)),
                pltpu.SemaphoreType.DMA((4,)),
                pltpu.SemaphoreType.DMA((n // 2,)),
                pltpu.SemaphoreType.DMA((2 * len(PIECES),)),
            ],
            compiler_params=pltpu.CompilerParams(
                collective_id=0, has_side_effects=True, vmem_limit_bytes=62000000
            ),
            name="mlp_ring",
        )(x, w_gate, w_up, w_down)

    return jax.shard_map(
        step,
        mesh=mesh,
        in_specs=(P(("dp", "tp"), None), P(None, "tp"), P(None, "tp"), P("tp", None)),
        out_specs=P(("dp", "tp"), None),
        check_vma=False,
    )
```
